256 devices in a mesh: cut: 32 (over z, y), sub: 8 (over x, core).
Axes of the slice: x: 4, y: 4, z: 8, core: 2. Of those that a mesh axis runs over, the one named last changes fastest.
Arguments:
- residual: bfloat16 [32, 8, 1024, 128], P('cut', 'sub'), may hold values from -6 to 6
- inner_inverse: bfloat16 [32, 8, 4, 343, 343], P('cut', 'sub'), may hold values from -0.3125 to 0.3125
- inner_index: int32 [32, 8, 4, 343], P('cut', 'sub'), may hold values from 0 to 1023
- slab_dofs: int32 [32, 8, 5, 512], P('cut', 'sub'), may hold values from 0 to 1023
- face_inverse: bfloat16 [32, 8, 5, 3, 343, 343], P('cut', 'sub'), may hold values from -0.3125 to 0.3125
- face_index: int32 [32, 8, 5, 3, 343], P('cut', 'sub'), may hold values from 0 to 1023
- face_count: int32 [32, 8, 5], P('cut', 'sub'), may hold values from 1 to 3
Outputs:
- correction: float32 [32, 8, 1024, 128], P('cut', 'sub')
The draws below stay inside these ranges and needn't reach their ends.
All inputs are finite; a program needn't handle non-finite values.
Results may differ from the reference program's by a relative error of at most 0.0003.
Values may be sent and summed in bfloat16 or wider, within the bound.
No kernel may reach another device: no remote copies, remote signals or barrier semaphores. Data moves between devices by JAX's collectives and lax.ppermute only.
A program may use at most 64 MiB of HBM per device.

```python
import jax
import jax.numpy as jnp
from jax import lax

STAR = 343
NDOF = 1024
NRHS = 128
NINT = 4
SLAB = 512
ISTAR = 3
CUTLV = 3
LEVELS = 5
PC = 32
PS = 8
N_CUT = 32
N_SUB = 8


def set_ends(entries, key, least, top_value):
    index_at = [jax.random.randint(jax.random.fold_in(key, axis), (), 0, length) for axis, length in enumerate(entries.shape)]
    longest = entries.shape.index(max(entries.shape))
    beside = index_at[:longest] + [(index_at[longest] + 1) % entries.shape[longest]] + index_at[longest + 1:]
    return entries.at[tuple(index_at)].set(least).at[tuple(beside)].set(top_value)


def shard_levels(stream_key, shape, shards, least, high):
    level = 1.0
    for axis_at, blocks in shards:
        heights = jax.random.uniform(jax.random.fold_in(jax.random.fold_in(stream_key, 6), axis_at), (blocks,), jnp.float32, least / len(shards), high / len(shards))
        level = level * jnp.repeat(jnp.exp(heights), shape[axis_at] // blocks).reshape((-1,) + (1,) * (len(shape) - 1 - axis_at))
    return level


def gaussian(key, extent, scale, bound, pieces=(), kind=jnp.bfloat16):
    drawn = scale * jax.random.normal(key, extent, jnp.float32)
    if pieces:
        drawn = drawn * shard_levels(key, extent, pieces, -0.22, 0.18)
    return jnp.clip(drawn, -bound, bound).astype(kind)


def setup_inputs(seed: int = 0) -> dict:
    keys = jax.random.split(jax.random.key(seed), 8)
    return {
        "residual": gaussian(keys[0], (PC, PS, NDOF, NRHS), 1.0, 6.0, ((0, 32), (1, 8))),
        "inner_inverse": gaussian(keys[1], (PC, PS, NINT, STAR, STAR), STAR ** -0.5, 0.3125, ((0, 32), (1, 8))),
        "inner_index": set_ends(jax.random.randint(keys[2], (PC, PS, NINT, STAR), 0, NDOF), jax.random.fold_in(keys[2], 1), 0, NDOF - 1).astype(jnp.int32),
        "slab_dofs": set_ends(jax.random.randint(keys[3], (PC, PS, LEVELS, SLAB), 0, NDOF), jax.random.fold_in(keys[3], 1), 0, NDOF - 1).astype(jnp.int32),
        "face_inverse": gaussian(keys[4], (PC, PS, LEVELS, ISTAR, STAR, STAR), STAR ** -0.5, 0.3125, ((0, 32), (1, 8))),
        "face_index": set_ends(jax.random.randint(keys[5], (PC, PS, LEVELS, ISTAR, STAR), 0, 2 * SLAB), jax.random.fold_in(keys[5], 1), 0, (2 * SLAB) - 1).astype(jnp.int32),
        "face_count": set_ends(jax.random.randint(keys[6], (PC, PS, LEVELS), 1, ISTAR + 1), jax.random.fold_in(keys[6], 1), 1, ISTAR).astype(jnp.int32),
    }


def star_apply(inverses, indices, live, source, row_count):
    gathered = jnp.take(source, indices, axis=0)
    solved = jnp.einsum("nij,njr->nir", inverses.astype(jnp.float32), gathered.astype(jnp.float32))
    solved = solved * live[:, None, None]
    width = source.shape[1]
    blank = jnp.zeros((row_count, width), jnp.float32)
    return blank.at[indices.reshape(-1)].add(solved.reshape(-1, width))


def reference(residual, inner_inverse, inner_index, slab_dofs, face_inverse, face_index, face_count):
    total_devices = PC * PS
    flat_residual = residual.reshape(total_devices, NDOF, NRHS)
    flat_inner_inv = inner_inverse.reshape(total_devices, NINT, STAR, STAR)
    flat_inner_idx = inner_index.reshape(total_devices, NINT, STAR)
    flat_dofs = slab_dofs.reshape(total_devices, LEVELS, SLAB)
    flat_face_inv = face_inverse.reshape(total_devices, LEVELS, ISTAR, STAR, STAR)
    flat_face_idx = face_index.reshape(total_devices, LEVELS, ISTAR, STAR)
    flat_count = face_count.reshape(total_devices, LEVELS)
    inner_live = jnp.ones((NINT,), jnp.float32)

    def inner_one(bundle):
        return star_apply(bundle[0], bundle[1], inner_live, bundle[2], NDOF)

    correction = lax.map(inner_one, (flat_inner_inv, flat_inner_idx, flat_residual))
    devices = jnp.arange(total_devices, dtype=jnp.int32)
    cut_index = devices // PS
    sub_index = devices % PS
    cut_bits = N_CUT.bit_length() - 1
    sub_bits = N_SUB.bit_length() - 1
    star_slots = jnp.arange(ISTAR, dtype=jnp.int32)
    for level in range(LEVELS):
        if level < CUTLV:
            shift_bit = cut_bits - 1 - level
            partner = (cut_index ^ (1 << shift_bit)) * PS + sub_index
            is_upper = (cut_index >> shift_bit) & 1
        else:
            shift_bit = sub_bits - 1 - (level - CUTLV)
            partner = cut_index * PS + (sub_index ^ (1 << shift_bit))
            is_upper = (sub_index >> shift_bit) & 1
        dofs_now = flat_dofs[:, level]
        own_slab = jax.vmap(lambda source, picked: jnp.take(source, picked, axis=0))(flat_residual, dofs_now)
        far_slab = own_slab[partner]
        upper_flag = (is_upper == 1)[:, None, None]
        joined = jnp.where(upper_flag, jnp.concatenate([far_slab, own_slab], axis=1), jnp.concatenate([own_slab, far_slab], axis=1))
        live = (star_slots[None, :] < flat_count[:, level][:, None]).astype(jnp.float32)

        def face_one(bundle):
            return star_apply(bundle[0], bundle[1], bundle[2], bundle[3], 2 * SLAB)

        terms = lax.map(face_one, (flat_face_inv[:, level], flat_face_idx[:, level], live, joined))
        paired = terms + terms[partner]
        slab_terms = jnp.where(upper_flag, paired[:, SLAB:], paired[:, :SLAB])
        correction = jax.vmap(lambda whole, picked, portion: whole.at[picked].add(portion))(correction, dofs_now, slab_terms)
    return correction.reshape(PC, PS, NDOF, NRHS)
```

```python
import functools

import jax
import jax.numpy as jnp
from jax import lax
from jax.experimental import pallas as pl
from jax.experimental.pallas import tpu as pltpu
from jax.sharding import PartitionSpec as P

CUTLV = 3
SUBLV = 2
LEVELS = CUTLV + SUBLV
BLK = 256
GRP = 64
VMEM = pltpu.VMEM
F32 = jnp.float32
BF16 = jnp.bfloat16


def partner(shard, axis, apart):
    return lax.ppermute(shard, axis, [(i, i ^ 1 << apart) for i in range(lax.axis_size(axis))])


def split_index(index):
    return index >> 8, (index & (BLK - 1)).astype(F32)


def one_hot(offset):
    rows = lax.broadcasted_iota(jnp.int32, (BLK, offset.shape[1]), 0).astype(F32).astype(BF16)
    return jnp.where(rows == offset.astype(BF16), BF16(1), BF16(0))


def pick_columns(stacked, index, group_count):
    group, offset = split_index(index)
    parts = jnp.dot(stacked, one_hot(offset), preferred_element_type=F32)
    width = stacked.shape[0] // group_count
    out = parts[:width]
    for g in range(1, group_count):
        out = jnp.where(group == g, parts[g * width : (g + 1) * width], out)
    return out


def group_one_hot(group, offset, g):
    return one_hot(jnp.where(group == g, offset, -1.0))


def hi_lo(value):
    hi = value.astype(BF16)
    return hi, (value - hi.astype(F32)).astype(BF16)


def slabs_kernel(v_ref, dofs_ref, *outs):
    stacked = jnp.concatenate(
        [v_ref[g * BLK : (g + 1) * BLK, :].astype(F32).T.astype(BF16) for g in range(4)], axis=0
    )
    for level, out in enumerate(outs):
        out[...] = pick_columns(stacked, dofs_ref[level], 4).astype(BF16)


def level_kernel(level, upper_of, own_ref, far_ref, m_ref, idx_ref, cnt_ref, kept_ref, given_ref, rhs):
    slots = m_ref.shape[1]
    star = m_ref.shape[2]
    wide = idx_ref.shape[2]
    flip = upper_of() * 512
    stacked = jnp.concatenate(
        [own_ref[:, :BLK], own_ref[:, BLK:], far_ref[:, :BLK], far_ref[:, BLK:]], axis=0
    )
    raw = jnp.concatenate([idx_ref[level * slots + j] for j in range(slots)], axis=1)
    index = raw ^ flip
    gathered = pick_columns(stacked, index, 4).astype(BF16)
    for j in range(slots):
        solved = lax.dot_general(
            m_ref[level, j],
            gathered[:, j * wide : j * wide + star],
            (((1,), (1,)), ((), ())),
            preferred_element_type=F32,
        )
        hi, lo = hi_lo(solved)
        rhs[j * wide : j * wide + star, :128] = hi
        rhs[j * wide : j * wide + star, 128:] = lo
        rhs[j * wide + star : (j + 1) * wide, :] = jnp.zeros((wide - star, 256), BF16)
    group, offset = split_index(index)
    place = lax.broadcasted_iota(jnp.int32, index.shape, 1)
    live = (raw >= 0) & (place < cnt_ref[level] * wide)
    group = jnp.where(live, group, -1)
    terms = []
    for g in range(4):
        both = jnp.dot(group_one_hot(group, offset, g), rhs[...], preferred_element_type=F32)
        terms.append(both[:, :128] + both[:, 128:])
    kept_ref[:256] = terms[0]
    kept_ref[256:] = terms[1]
    far = jnp.concatenate(terms[2:], axis=0)
    pack(far, given_ref)


def pack(value, out_ref):
    rows, cols = value.shape
    groups = rows // GRP
    parts = [value[g * GRP : (g + 1) * GRP] for g in range(groups)]
    top = jnp.concatenate([jnp.max(jnp.abs(p), axis=0, keepdims=True) for p in parts], axis=0)
    power = jnp.ceil(jnp.log2(jnp.clip(top, 1e-30, 1e30)))
    scale = jnp.exp2(15.0 - power)
    for g, p in enumerate(parts):
        q = jnp.clip(jnp.round(p * scale[g : g + 1]), -32767.0, 32767.0)
        out_ref[g * GRP : (g + 1) * GRP] = q.astype(jnp.int32).astype(jnp.int16)
    code = jnp.concatenate([power, jnp.zeros((16 - groups, cols), F32)], axis=0)
    out_ref[rows : rows + 16] = code.astype(jnp.int32).astype(jnp.int16)


def unpack(ref):
    rows = ref.shape[0] - 16
    groups = rows // GRP
    power = ref[rows : rows + 16].astype(jnp.int32).astype(F32)
    scale = jnp.exp2(power - 15.0)
    return jnp.concatenate(
        [
            ref[g * GRP : (g + 1) * GRP].astype(jnp.int32).astype(F32) * scale[g : g + 1]
            for g in range(groups)
        ],
        axis=0,
    )


def inner_kernel(solved_ref, idx_ref, out_ref, rhs):
    stars, star, _ = solved_ref.shape
    wide = idx_ref.shape[2]
    for n in range(stars):
        hi, lo = hi_lo(solved_ref[n])
        rhs[n * wide : n * wide + star, :128] = hi
        rhs[n * wide : n * wide + star, 128:] = lo
        rhs[n * wide + star : (n + 1) * wide, :] = jnp.zeros((wide - star, 256), BF16)
    raw = jnp.concatenate([idx_ref[n] for n in range(stars)], axis=1)
    group, offset = split_index(raw)
    for g in range(4):
        both = jnp.dot(group_one_hot(group, offset, g), rhs[...], preferred_element_type=F32)
        out_ref[g * BLK : (g + 1) * BLK] = both[:, :128] + both[:, 128:]


def finish_kernel(levels, base_ref, dofs_ref, *refs):
    kept = refs[: len(levels)]
    got = refs[len(levels) : 2 * len(levels)]
    out_ref, rhs = refs[2 * len(levels) :]
    for n in range(len(levels)):
        hi, lo = hi_lo(kept[n][...] + unpack(got[n]))
        rhs[n * 512 : (n + 1) * 512, :128] = hi
        rhs[n * 512 : (n + 1) * 512, 128:] = lo
    index = jnp.concatenate([dofs_ref[level] for level in levels], axis=1)
    group, offset = split_index(index)
    for g in range(4):
        both = jnp.dot(group_one_hot(group, offset, g), rhs[...], preferred_element_type=F32)
        rows = slice(g * BLK, (g + 1) * BLK)
        out_ref[rows] = base_ref[rows] + both[:, :128] + both[:, 128:]


def call(body, out_shape, ins, scratch=(), smem=(), flops=2_000_000_000, name=None):
    specs = [
        pl.BlockSpec(memory_space=pltpu.SMEM if n in smem else VMEM) for n in range(len(ins))
    ]
    outs = jax.tree.map(lambda _: pl.BlockSpec(memory_space=VMEM), out_shape)
    return pl.pallas_call(
        body,
        out_shape=out_shape,
        in_specs=specs,
        out_specs=outs,
        scratch_shapes=list(scratch),
        compiler_params=pltpu.CompilerParams(vmem_limit_bytes=24 << 20),
        cost_estimate=pl.CostEstimate(flops=flops, bytes_accessed=1 << 20, transcendentals=0),
        name=name,
    )(*ins)


def pad_index(index, wide):
    return jnp.pad(index, ((0, 0), (0, wide - index.shape[1])), constant_values=-1)[:, None, :]


def on_device(
    residual, inner_inverse, inner_index, slab_dofs, face_inverse, face_index, face_count
):
    shape = jax.ShapeDtypeStruct
    source = residual[0, 0]
    rows, cols = source.shape
    levels, slab = slab_dofs.shape[2:]
    slots, star = face_index.shape[3:]
    wide = -(-star // 128) * 128
    dofs = slab_dofs[0, 0][:, None, :]
    faces_inv = face_inverse[0, 0]
    faces_idx = pad_index(face_index[0, 0].reshape(levels * slots, star), wide)
    inner_idx = pad_index(inner_index[0, 0], wide)
    counts = face_count[0, 0]
    slabs = call(
        slabs_kernel,
        [shape((cols, slab), BF16)] * levels,
        (source, dofs),
        name="slabs",
    )
    cut_bits = lax.axis_size("cut").bit_length() - 1
    sub_bits = lax.axis_size("sub").bit_length() - 1
    route = [("cut", cut_bits - 1 - k) for k in range(CUTLV)]
    route += [("sub", sub_bits - 1 - k) for k in range(SUBLV)]
    far = [partner(slabs[k], *route[k]) for k in range(levels)]

    selector = (inner_index[0, 0][..., None] == jnp.arange(rows, dtype=jnp.int32)).astype(BF16)
    gathered = jnp.einsum("nsd,dr->nsr", selector, source, preferred_element_type=F32).astype(BF16)
    solved = jnp.einsum("nij,njr->nir", inner_inverse[0, 0], gathered, preferred_element_type=F32)
    stars = solved.shape[0]
    inner = call(
        inner_kernel,
        shape((rows, cols), F32),
        (solved, inner_idx),
        scratch=[pltpu.VMEM((stars * wide, 256), BF16)],
        name="inner",
    )

    kept, got = [None] * levels, [None] * levels
    for k in range(levels):
        axis, bit = route[k]
        kept[k], given = call(
            functools.partial(level_kernel, k, lambda: lax.axis_index(axis) >> bit & 1),
            (shape((slab, cols), F32), shape((slab + 16, cols), jnp.int16)),
            (slabs[k], far[k], faces_inv, faces_idx, counts),
            scratch=[pltpu.VMEM((slots * wide, 256), BF16)],
            smem=(4,),
            name=f"level{k}",
        )
        got[k] = partner(given, axis, bit)

    out = call(
        functools.partial(finish_kernel, tuple(range(levels))),
        shape((rows, cols), F32),
        (inner, dofs, *kept, *got),
        scratch=[pltpu.VMEM((levels * slab, 256), BF16)],
        name="finish",
    )
    return out[None, None]


def solution(mesh):
    return jax.shard_map(
        on_device,
        mesh=mesh,
        in_specs=(
            P("cut", "sub", None, None),
            P("cut", "sub", None, None, None),
            P("cut", "sub", None, None),
            P("cut", "sub", None, None),
            P("cut", "sub", None, None, None, None),
            P("cut", "sub", None, None, None),
            P("cut", "sub", None),
        ),
        out_specs=P("cut", "sub", None, None),
        check_vma=False,
    )
```

```python
import functools

import jax
import jax.numpy as jnp
from jax import lax
from jax.experimental import pallas as pl
from jax.experimental.pallas import tpu as pltpu
from jax.sharding import PartitionSpec as P


CUTLV = 3
SUBLV = 2
BLK = 256
GRP = 64
ORDER = (4, 0, 1, 2, 3)
VMEM = pltpu.VMEM
F32 = jnp.float32
BF16 = jnp.bfloat16


def partner(shard, axis, apart):
    return lax.ppermute(shard, axis, [(i, i ^ 1 << apart) for i in range(lax.axis_size(axis))])


def lanes(row, wide):
    return jnp.concatenate([row, jnp.full((1, wide - row.shape[1]), -1, jnp.int32)], axis=1)


def split_index(index):
    return index >> 8, (index & (BLK - 1)).astype(F32)


def one_hot(offset):
    rows = lax.broadcasted_iota(jnp.int32, (BLK, offset.shape[1]), 0).astype(F32).astype(BF16)
    return jnp.where(rows == offset.astype(BF16), BF16(1), BF16(0))


def pick_columns(stacked, index, group_count):
    group, offset = split_index(index)
    parts = jnp.dot(stacked, one_hot(offset), preferred_element_type=F32)
    width = stacked.shape[0] // group_count
    out = parts[:width]
    for g in range(1, group_count):
        out = jnp.where(group == g, parts[g * width : (g + 1) * width], out)
    return out


def group_one_hot(group, offset, g):
    return one_hot(jnp.where(group == g, offset, -1.0))


def hi_lo(value):
    hi = value.astype(BF16)
    return hi, (value - hi.astype(F32)).astype(BF16)


def stack_kernel(v_ref, out_ref):
    rows, cols = v_ref.shape
    for g in range(rows // BLK):
        out_ref[g * cols : (g + 1) * cols] = v_ref[g * BLK : (g + 1) * BLK].astype(F32).T.astype(BF16)


def slabs_kernel(stacked_ref, dofs_ref, *outs):
    stacked = stacked_ref[...]
    for level, out in enumerate(outs):
        out[...] = pick_columns(stacked, dofs_ref[level], 4).astype(BF16)


def level_kernel(level, upper_of, own_ref, far_ref, m_ref, idx_ref, cnt_ref, kept_ref, given_ref, rhs):
    slots = m_ref.shape[1]
    star = m_ref.shape[2]
    wide = rhs.shape[0] // slots
    flip = upper_of() * 512
    stacked = jnp.concatenate(
        [own_ref[:, :BLK], own_ref[:, BLK:], far_ref[:, :BLK], far_ref[:, BLK:]], axis=0
    )
    raw = jnp.concatenate([lanes(idx_ref[level * slots + j], wide) for j in range(slots)], axis=1)
    index = raw ^ flip
    gathered = pick_columns(stacked, index, 4).astype(BF16)
    for j in range(slots):
        solved = lax.dot_general(
            m_ref[level, j],
            gathered[:, j * wide : j * wide + star],
            (((1,), (1,)), ((), ())),
            preferred_element_type=F32,
        )
        hi, lo = hi_lo(solved)
        rhs[j * wide : j * wide + star, :128] = hi
        rhs[j * wide : j * wide + star, 128:] = lo
        rhs[j * wide + star : (j + 1) * wide, :] = jnp.zeros((wide - star, 256), BF16)
    group, offset = split_index(index)
    place = lax.broadcasted_iota(jnp.int32, index.shape, 1)
    live = (raw >= 0) & (place < cnt_ref[level] * wide)
    group = jnp.where(live, group, -1)
    terms = []
    for g in range(4):
        both = jnp.dot(group_one_hot(group, offset, g), rhs[...], preferred_element_type=F32)
        terms.append(both[:, :128] + both[:, 128:])
    kept_ref[:256] = terms[0]
    kept_ref[256:] = terms[1]
    far = jnp.concatenate(terms[2:], axis=0)
    pack(far, given_ref)


def pack(value, out_ref):
    rows, cols = value.shape
    groups = rows // GRP
    parts = [value[g * GRP : (g + 1) * GRP] for g in range(groups)]
    top = jnp.concatenate([jnp.max(jnp.abs(p), axis=0, keepdims=True) for p in parts], axis=0)
    power = jnp.ceil(jnp.log2(jnp.clip(top, 1e-30, 1e30)))
    scale = jnp.exp2(15.0 - power)
    for g, p in enumerate(parts):
        q = jnp.clip(jnp.round(p * scale[g : g + 1]), -32767.0, 32767.0)
        out_ref[g * GRP : (g + 1) * GRP] = q.astype(jnp.int32).astype(jnp.int16)
    code = jnp.concatenate([power, jnp.zeros((16 - groups, cols), F32)], axis=0)
    out_ref[rows : rows + 16] = code.astype(jnp.int32).astype(jnp.int16)


def unpack(ref):
    rows = ref.shape[0] - 16
    groups = rows // GRP
    power = ref[rows : rows + 16].astype(jnp.int32).astype(F32)
    scale = jnp.exp2(power - 15.0)
    return jnp.concatenate(
        [
            ref[g * GRP : (g + 1) * GRP].astype(jnp.int32).astype(F32) * scale[g : g + 1]
            for g in range(groups)
        ],
        axis=0,
    )


def inner_kernel(stacked_ref, m_ref, idx_ref, out_ref, terms, rhs):
    star, stars, _ = m_ref.shape
    wide = rhs.shape[0] // stars
    raw = jnp.concatenate([lanes(idx_ref[n : n + 1, :], wide) for n in range(stars)], axis=1)
    gathered = pick_columns(stacked_ref[...], raw, 4).astype(BF16)
    every = lax.dot_general(
        m_ref[...].reshape(star * stars, star),
        jnp.concatenate([gathered[:, n * wide : n * wide + star] for n in range(stars)], axis=0),
        (((1,), (1,)), ((), ())),
        preferred_element_type=F32,
    )
    row_star = lax.rem(lax.broadcasted_iota(jnp.int32, (star * stars, 128), 0), stars)
    own = every[:, :128]
    for n in range(1, stars):
        own = jnp.where(row_star == n, every[:, n * 128 : (n + 1) * 128], own)
    terms[...] = own
    for n in range(stars):
        hi, lo = hi_lo(terms[pl.ds(n, star, stride=stars), :])
        rhs[n * wide : n * wide + star, :128] = hi
        rhs[n * wide : n * wide + star, 128:] = lo
        rhs[n * wide + star : (n + 1) * wide, :] = jnp.zeros((wide - star, 256), BF16)
    group, offset = split_index(raw)
    for g in range(4):
        both = jnp.dot(group_one_hot(group, offset, g), rhs[...], preferred_element_type=F32)
        out_ref[g * BLK : (g + 1) * BLK] = both[:, :128] + both[:, 128:]


def finish_kernel(levels, base_ref, dofs_ref, *refs):
    kept = refs[: len(levels)]
    got = refs[len(levels) : 2 * len(levels)]
    out_ref, rhs = refs[2 * len(levels) :]
    for n in range(len(levels)):
        hi, lo = hi_lo(kept[n][...] + unpack(got[n]))
        rhs[n * 512 : (n + 1) * 512, :128] = hi
        rhs[n * 512 : (n + 1) * 512, 128:] = lo
    index = jnp.concatenate([dofs_ref[level] for level in levels], axis=1)
    group, offset = split_index(index)
    for g in range(4):
        both = jnp.dot(group_one_hot(group, offset, g), rhs[...], preferred_element_type=F32)
        rows = slice(g * BLK, (g + 1) * BLK)
        out_ref[rows] = base_ref[rows] + both[:, :128] + both[:, 128:]


def call(body, out_shape, ins, scratch=(), smem=(), flops=2_000_000_000):
    specs = [
        pl.BlockSpec(memory_space=pltpu.SMEM if n in smem else VMEM)
        for n in range(len(ins))
    ]
    outs = jax.tree.map(lambda _: pl.BlockSpec(memory_space=VMEM), out_shape)
    return pl.pallas_call(
        body,
        out_shape=out_shape,
        in_specs=specs,
        out_specs=outs,
        scratch_shapes=list(scratch),
        compiler_params=pltpu.CompilerParams(vmem_limit_bytes=24 << 20),
        cost_estimate=pl.CostEstimate(flops=flops, bytes_accessed=1 << 20, transcendentals=0),
    )(*ins)


def on_device(
    residual, inner_inverse, inner_index, slab_dofs, face_inverse, face_index, face_count
):
    shape = jax.ShapeDtypeStruct
    source = residual[0, 0]
    rows, cols = source.shape
    levels, slab = slab_dofs.shape[2:]
    slots, star = face_index.shape[3:]
    wide = -(-star // 128) * 128
    dofs = slab_dofs[0, 0][:, None, :]
    faces_inv = face_inverse[0, 0]
    faces_idx = face_index.reshape(levels * slots, 1, star)
    stars = inner_index.shape[2]
    counts = face_count[0, 0]
    stacked = call(stack_kernel, shape((rows // BLK * cols, BLK), BF16), (source,))
    slabs = call(slabs_kernel, [shape((cols, slab), BF16)] * levels, (stacked, dofs))
    cut_bits = lax.axis_size("cut").bit_length() - 1
    sub_bits = lax.axis_size("sub").bit_length() - 1
    route = [("cut", cut_bits - 1 - k) for k in range(CUTLV)]
    route += [("sub", sub_bits - 1 - k) for k in range(SUBLV)]
    far = []
    for k in range(levels):
        far.append(partner(slabs[k], *route[k]))

    kept, got = [None] * levels, [None] * levels
    for k in ORDER:
        axis, bit = route[k]
        kept[k], given = call(
            functools.partial(level_kernel, k, lambda: lax.axis_index(axis) >> bit & 1),
            (shape((slab, cols), F32), shape((slab + 16, cols), jnp.int16)),
            (slabs[k], far[k], faces_inv, faces_idx, counts),
            scratch=[pltpu.VMEM((slots * wide, 256), BF16)],
            smem=(4,),
        )
        got[k] = partner(given, axis, bit)

    out = call(
        inner_kernel,
        shape((rows, cols), F32),
        (stacked, jnp.transpose(inner_inverse[0, 0], (1, 0, 2)), inner_index[0, 0]),
        scratch=[
            pltpu.VMEM((star * stars, cols), F32),
            pltpu.VMEM((stars * wide, 256), BF16),
        ],
    )
    for part in (ORDER[:-1], ORDER[-1:]):
        out = call(
            functools.partial(finish_kernel, part),
            shape((rows, cols), F32),
            (out, dofs, *(kept[k] for k in part), *(got[k] for k in part)),
            scratch=[pltpu.VMEM((len(part) * slab, 256), BF16)],
        )
    return out[None, None]


def solution(mesh):
    return jax.shard_map(
        on_device,
        mesh=mesh,
        in_specs=(
            P("cut", "sub", None, None),
            P("cut", "sub", None, None, None),
            P("cut", "sub", None, None),
            P("cut", "sub", None, None),
            P("cut", "sub", None, None, None, None),
            P("cut", "sub", None, None, None),
            P("cut", "sub", None),
        ),
        out_specs=P("cut", "sub", None, None),
        check_vma=False,
    )
```
